128 devices in a mesh: shot: 8 (over x_lo, z), gx: 4 (over y), gy: 4 (over x_hi, core).
Axes of the slice: x: 4 (x_hi: 2, x_lo: 2; x = x_hi * 2 + x_lo), y: 4, z: 4, core: 2. Of those that a mesh axis runs over, the one named last changes fastest.
Arguments:
- forward: bfloat16 [8, 2, 9, 16, 512, 512], P('shot', None, None, None, 'gx', 'gy'), may hold values from -6 to 6
- adjoint: bfloat16 [8, 2, 9, 16, 512, 512], P('shot', None, None, None, 'gx', 'gy'), may hold values from -6 to 6
- snap_times: int32 [8, 2], P('shot'), may hold values from 1 to 32, as said below
- sources: int32 [8, 2], P('shot'), may hold values from 0 to 511
- aperture: int32 [8, 4, 4], P('shot', 'gx', 'gy'), may hold values 0 or 1
Outputs:
- smoothed: float32 [3, 16, 512, 512], P(None, 'shot', 'gx', 'gy')
The draws below stay inside these ranges and needn't reach their ends.
Inputs may be any that keep to these rules, and one draw needn't show every extreme that they name: `snap_times`: each shot's times rise strictly, the first and every step from one to the next being 1 to 16; some shot takes steps of 16 throughout.
All inputs are finite; a program needn't handle non-finite values. No bound on the sum of `aperture` on one device may be relied on, other than what follows from the above.
Results may differ from the reference program's by a relative error of at most 0.0003.
Values sent between devices are 32-bit elements; how exact they have to be, the bound alone decides.
No kernel may reach another device: no remote copies, remote signals or barrier semaphores. Data moves between devices by JAX's collectives and lax.ppermute only.
A program may use at most 64 MiB of HBM per device.

```python
import jax
import jax.numpy as jnp
from jax import lax

CX = 128
CY = 128
LEV = 16
SNAPS = 2
COMPS = 9
RADIUS = 16
SHOTS = 8
NX = 512
NY = 512
MUTE = 32
N_GX = 4
N_GY = 4


def draw_snap_times(key, part):
    step_sizes = jax.random.randint(jax.random.fold_in(key, 11), (SHOTS, SNAPS), 1, 17)
    full_shot = jax.random.randint(jax.random.fold_in(key, 12), (), 0, SHOTS)
    short_shot = (full_shot + 1) % SHOTS
    shot_ids = jnp.arange(SHOTS)[:, None]
    snap_ids = jnp.arange(SNAPS)[None, :]
    step_sizes = jnp.where(shot_ids == full_shot, 16, step_sizes)
    step_sizes = jnp.where((shot_ids == short_shot) & (snap_ids == 0), 1, step_sizes)
    return jnp.cumsum(step_sizes, axis=1).astype(jnp.int32)


def plant(drawn, own_key, low, top_value):
    shape = drawn.shape
    index_at = [jax.random.randint(jax.random.fold_in(own_key, axis), (), 0, shape[axis]) for axis in range(len(shape))]
    drawn = drawn.at[tuple(index_at)].set(low)
    longest = shape.index(max(shape))
    index_at[longest] = (index_at[longest] + 1) % shape[longest]
    return drawn.at[tuple(index_at)].set(top_value)


def strengthened(array, key, source, target, parts, factor):
    owner, partner = [(jnp.arange(array.shape[dim]) // (array.shape[dim] // parts)).reshape([-1 if axis == dim else 1 for axis in range(array.ndim)]) for dim in (source, target)]
    chosen = jax.random.permutation(key, parts)[partner]
    strong = (owner == chosen) | (owner == (partner + parts // 2) % parts)
    return jnp.where(strong, factor * array, array)


def block_scale(own_key, extent, cuts, smallest, largest):
    def one(axis_at, blocks):
        steps = jax.random.uniform(jax.random.fold_in(jax.random.fold_in(own_key, 6), axis_at), (blocks,), jnp.float32, smallest / len(cuts), largest / len(cuts))
        return jnp.repeat(jnp.exp(steps), extent[axis_at] // blocks).reshape((-1,) + (1,) * (len(extent) - axis_at - 1))

    level = one(*cuts[0])
    for cut in cuts[1:]:
        level = level * one(*cut)
    return level


def scatter_about(rng, shape, scale, most, shards=(), kind=jnp.bfloat16):
    drawn = jax.random.normal(rng, shape, jnp.float32) * scale
    if len(shards) > 0:
        drawn = block_scale(rng, shape, shards, -0.22, 0.18) * drawn
    return jnp.clip(drawn, min=-most, max=most).astype(kind)


def heavy_noise(stream_key, extent, scale, most, pieces, heavy, held_as=jnp.bfloat16):
    entries = scale * jax.random.normal(stream_key, extent, jnp.float32)
    if pieces:
        entries = entries * block_scale(stream_key, extent, pieces, -0.22, 0.18)
    return jnp.clip(strengthened(entries, jax.random.fold_in(stream_key, 3), *heavy), -most, most).astype(held_as)


def setup_inputs(seed: int = 0) -> dict:
    key_list = jax.random.split(jax.random.key(seed), 6)
    return {
        "forward": heavy_noise(key_list[0], (SHOTS, SNAPS, COMPS, LEV, NX, NY), 1.0, 6.0, ((0, 8), (4, 4), (5, 4)), (0, 3, 8, 2.0)),
        "adjoint": scatter_about(key_list[1], (SHOTS, SNAPS, COMPS, LEV, NX, NY), 1.0, 6.0, ((0, 8), (4, 4), (5, 4))),
        "snap_times": draw_snap_times(jax.random.fold_in(key_list[5], 71), 0),
        "sources": plant(jax.random.randint(key_list[3], (SHOTS, 2), 0, min(NX, NY)), jax.random.fold_in(key_list[3], 1), 0, (min(NX, NY)) - 1).astype(jnp.int32),
        "aperture": plant((jax.random.randint(key_list[4], (SHOTS, N_GX, N_GY), 0, 4) < 3).astype(jnp.int32), jax.random.fold_in(key_list[4], 1), 0, 1),
    }


spread_x = 0.5
spread_y = 0.375


def kernel_weights(sigma):
    tap_list = jnp.arange(-RADIUS, RADIUS + 1).astype(jnp.float32)
    raw_taps = jnp.exp(-tap_list * tap_list / (2.0 * sigma * sigma))
    return raw_taps / jnp.sum(raw_taps)


def shot_gradient(forward_shot, adjoint_shot, steps_here, source, mask_tile):
    earlier = jnp.concatenate([jnp.zeros((1,), jnp.int32), steps_here[:-1]])
    weights = (steps_here - earlier).astype(jnp.float32) / 8.0
    gradient = jnp.zeros((3, LEV, NX, NY), jnp.float32)
    for which in range(SNAPS):
        forward_now = forward_shot[which]
        adjoint_now = adjoint_shot[which]

        def product(comp):
            return forward_now[comp].astype(jnp.float32) * adjoint_now[comp].astype(jnp.float32)

        density_term = product(0) + product(1) + product(2)
        trace_fwd = forward_now[3].astype(jnp.float32) + forward_now[4].astype(jnp.float32) + forward_now[5].astype(jnp.float32)
        trace_adj = adjoint_now[3].astype(jnp.float32) + adjoint_now[4].astype(jnp.float32) + adjoint_now[5].astype(jnp.float32)
        lame_term = trace_fwd * trace_adj
        shear_term = 2.0 * (product(3) + product(4) + product(5) + 2.0 * (product(6) + product(7) + product(8)))
        gradient = gradient + jnp.stack([lame_term, shear_term, density_term]) * (-weights[which])
    x_cells = jnp.arange(NX).astype(jnp.int32)
    y_cells = jnp.arange(NY).astype(jnp.int32)
    delta_x = (x_cells - source[0]).astype(jnp.float32)
    delta_y = (y_cells - source[1]).astype(jnp.float32)
    distance = (delta_x * delta_x)[:, None] + (delta_y * delta_y)[None, :]
    mask_cells = jnp.repeat(jnp.repeat(mask_tile, CX, 0), CY, 1).astype(jnp.float32)
    taper = (1.0 - jnp.exp(-distance / (2.0 * MUTE * MUTE))) * mask_cells
    return gradient * taper


def reference(forward, adjoint, snap_times, sources, aperture):
    def add_shot(carry, items):
        return carry + shot_gradient(*items), None

    start = jnp.zeros((3, LEV, NX, NY), jnp.float32)
    total, _ = lax.scan(add_shot, start, (forward, adjoint, snap_times, sources, aperture))
    weights_x = kernel_weights(spread_x * RADIUS)
    padded = jnp.pad(total, ((0, 0), (0, 0), (RADIUS, RADIUS), (0, 0)))
    along_x = jnp.zeros_like(total)
    for shift in range(2 * RADIUS + 1):
        along_x = along_x + weights_x[shift] * padded[:, :, shift:shift + NX, :]
    weights_y = kernel_weights(spread_y * RADIUS)
    padded = jnp.pad(along_x, ((0, 0), (0, 0), (0, 0), (RADIUS, RADIUS)))
    smoothed = jnp.zeros_like(total)
    for shift in range(2 * RADIUS + 1):
        smoothed = smoothed + weights_y[shift] * padded[:, :, :, shift:shift + NY]
    return smoothed
```

```python
import functools

import jax
import jax.numpy as jnp
from jax import lax
from jax.experimental import pallas as pl
from jax.experimental.pallas import tpu as pltpu
from jax.sharding import PartitionSpec as P

RADIUS = 16
MUTE = 32
RZ = 4
CHUNK = 32

spread_x = 0.5
spread_y = 0.375


def gradient_kernel(steps, n_out, *refs):
    fwd, adj, small = refs[:3]
    outs = refs[3 : 3 + n_out]
    rest = list(refs[3 + n_out :])
    taper = rest.pop(0)
    sems = rest.pop(0)
    bufs = rest
    shot = lax.axis_index("shot")
    xl, z = lax.div(shot, RZ), lax.rem(shot, RZ)
    copies = []
    for n, (c0, cn, other, j, _) in enumerate(steps):
        half = 1 - xl if other else xl
        lev = 2 * (half * RZ + lax.rem(z + j, RZ))
        pair = []
        for a, src in enumerate((fwd, adj)):
            cp = pltpu.make_async_copy(
                src.at[0, :, pl.ds(c0, cn), pl.ds(lev, 2)], bufs[n].at[a], sems.at[n, a]
            )
            pair.append(cp)
        copies.append(pair)
    for pair in copies:
        for cp in pair:
            cp.start()
    t0, t1 = small[:, 0:1], small[:, 1:2]
    w0 = -(t0.astype(jnp.float32) / 8.0)
    w1 = -((t1 - t0).astype(jnp.float32) / 8.0)
    inside = small[:, 4:5].astype(jnp.float32)
    shape = taper.shape
    xs = lax.broadcasted_iota(jnp.int32, shape, 0) + lax.axis_index("gx") * shape[0]
    ys = lax.broadcasted_iota(jnp.int32, shape, 1) + lax.axis_index("gy") * shape[1]
    dx = (xs - small[:, 2:3]).astype(jnp.float32)
    dy = (ys - small[:, 3:4]).astype(jnp.float32)
    taper[...] = (1.0 - jnp.exp(-(dx * dx + dy * dy) / (2.0 * MUTE * MUTE))) * inside
    rows = shape[0]
    for n, (c0, cn, other, j, where) in enumerate(steps):
        for cp in copies[n]:
            cp.wait()
        buf = bufs[n]

        def body(i, carry, buf=buf, c0=c0, where=where):
            lev = lax.div(i, rows // CHUNK)
            r = pl.multiple_of(lax.rem(i, rows // CHUNK) * CHUNK, CHUNK)

            def load(a, k, c):
                return buf[a, k, c, lev, pl.ds(r, CHUNK), :].astype(jnp.float32)

            sums = None
            for k, w in ((0, w0), (1, w1)):
                if c0 == 0:
                    terms = [
                        load(0, k, 0) * load(1, k, 0)
                        + load(0, k, 1) * load(1, k, 1)
                        + load(0, k, 2) * load(1, k, 2)
                    ]
                else:
                    f = [load(0, k, c) for c in range(3)]
                    a = [load(1, k, c) for c in range(3)]
                    lame = (f[0] + f[1] + f[2]) * (a[0] + a[1] + a[2])
                    shear = f[0] * a[0] + f[1] * a[1] + f[2] * a[2]
                    cross = (
                        load(0, k, 3) * load(1, k, 3)
                        + load(0, k, 4) * load(1, k, 4)
                        + load(0, k, 5) * load(1, k, 5)
                    )
                    terms = [lame, 2.0 * (shear + 2.0 * cross)]
                terms = [t * w for t in terms]
                sums = terms if sums is None else [s + t for s, t in zip(sums, terms)]
            mask = taper[pl.ds(r, CHUNK), :]
            for s, (o, i_o) in zip(sums, where):
                outs[o][i_o, lev, pl.ds(r, CHUNK), :] = s * mask
            return carry

        lax.fori_loop(0, 2 * (rows // CHUNK), body, 0)


def gradient(args, steps, counts, name):
    wx, wy = args[0].shape[4:]
    hbm = pl.BlockSpec(memory_space=pltpu.HBM)
    vm = pl.BlockSpec(memory_space=pltpu.VMEM)
    return pl.pallas_call(
        functools.partial(gradient_kernel, steps, len(counts)),
        out_shape=[pltpu.VMEM((c, 2, wx, wy), jnp.float32) for c in counts],
        in_specs=[hbm, hbm, vm],
        out_specs=[vm] * len(counts),
        scratch_shapes=[
            pltpu.VMEM((wx, wy), jnp.float32),
            pltpu.SemaphoreType.DMA((len(steps), 2)),
        ]
        + [pltpu.VMEM((2, 2, s[1], 2, wx, wy), jnp.bfloat16) for s in steps],
        compiler_params=pltpu.CompilerParams(vmem_limit_bytes=24 << 20),
        name=name,
    )(*args)


def band(out_first, sigma, count, extra):
    rows = lax.broadcasted_iota(jnp.int32, (count + extra, count), 0)
    cols = lax.broadcasted_iota(jnp.int32, (count + extra, count), 1)
    offset = rows - cols - extra // 2
    real = offset.astype(jnp.float32)
    taps = lax.broadcasted_iota(jnp.int32, (8, 128), 1) - RADIUS
    taps_real = taps.astype(jnp.float32)
    raw = jnp.where(
        taps <= RADIUS, jnp.exp(-taps_real * taps_real / (2.0 * sigma * sigma)), 0.0
    )
    total = jnp.sum(raw[0:1, :], axis=1, keepdims=True)
    values = jnp.exp(-real * real / (2.0 * sigma * sigma)) / total
    return jnp.where(jnp.abs(offset) <= RADIUS, values, 0.0)


def smooth_kernel(sigma, before, mid, after, out):
    width = mid.shape[-2]
    weights = band(0, sigma, width, 2 * RADIUS)
    for p in range(mid.shape[0]):
        cells = jnp.concatenate([before[p], mid[p], after[p]], axis=0)
        out[p] = lax.dot_general(
            cells,
            weights,
            (((0,), (0,)), ((), ())),
            precision=lax.Precision.HIGHEST,
            preferred_element_type=jnp.float32,
        )


def smooth(before, mid, after, sigma, name):
    vm = pl.BlockSpec(memory_space=pltpu.VMEM)
    n, r, c = mid.shape
    return pl.pallas_call(
        functools.partial(smooth_kernel, sigma),
        out_shape=jax.ShapeDtypeStruct((n, c, r), jnp.float32),
        in_specs=[vm] * 3,
        out_specs=vm,
        compiler_params=pltpu.CompilerParams(vmem_limit_bytes=16 << 20),
        name=name,
    )(before, mid, after)


def z_moves(shots, step):
    return [(h * RZ + k, h * RZ + (k + step) % RZ) for h in range(shots // RZ) for k in range(RZ)]


def halo(cells, axis):
    count = lax.axis_size(axis)
    head, tail = cells[:, :RADIUS], cells[:, -RADIUS:]
    before = lax.ppermute(tail, axis, [(i, i + 1) for i in range(count - 1)])
    after = lax.ppermute(head, axis, [(i + 1, i) for i in range(count - 1)])
    return before, after


def on_device(forward, adjoint, snap_times, sources, aperture):
    forward = pltpu.with_memory_space_constraint(forward, pltpu.HBM)
    adjoint = pltpu.with_memory_space_constraint(adjoint, pltpu.HBM)
    small = jnp.concatenate([snap_times, sources, aperture.reshape(1, 1)], axis=1)
    args = (forward, adjoint, small)

    def later(first):
        return forward, adjoint, lax.optimization_barrier((small, first))[0]

    shots = lax.axis_size("shot")
    up, down = z_moves(shots, 1), z_moves(shots, -1)
    across = [(i, (i + RZ) % shots) for i in range(shots)]

    def to_up(v):
        return lax.ppermute(v, "shot", up)

    def to_down(v):
        return lax.ppermute(v, "shot", down)

    def to_pair(v):
        return lax.ppermute(v, "shot", across)

    lame2, shear2 = gradient(
        args, [(3, 6, h, 2, ((0, h), (1, h))) for h in range(2)], (2, 2), "far"
    )
    lame2_in = to_up(lame2)
    shear2_in = to_down(shear2)
    lame1, shear1, lame3, shear3 = gradient(
        later(lame2),
        [(3, 6, h, 1, ((0, h), (1, h))) for h in range(2)]
        + [(3, 6, h, 3, ((2, h), (3, h))) for h in range(2)],
        (2, 2, 2, 2),
        "near",
    )
    shear_up_in = to_up(shear1)
    lame_down_in = to_down(lame3)
    density_other, = gradient(
        later(lame1), [(0, 3, 1, j, ((0, j),)) for j in range(RZ)], (RZ,), "density_other"
    )
    density_in = to_pair(density_other)
    lame0, shear0, density_own = gradient(
        later(density_other),
        [(3, 6, h, 0, ((0, h), (1, h))) for h in range(2)]
        + [(0, 3, 0, j, ((2, j),)) for j in range(RZ)],
        (2, 2, RZ),
        "own",
    )
    lame_up_in = to_up(lame1 + lame2_in)
    shear_down_in = to_down(shear3 + shear2_in)
    lame = lame0 + lame_up_in + lame_down_in
    shear = shear0 + shear_up_in + shear_down_in
    pair_in = to_pair(jnp.stack([lame[1], shear[1]]))
    density = density_own + density_in
    first_up = to_up(jnp.stack([density[2, 0], density[1, 1]]))
    first_down = to_down(jnp.stack([density[2, 1], density[3, 0]]))
    sum_up = to_up(density[1, 0:1] + first_up[0:1])
    sum_down = to_down(density[3, 1:2] + first_down[0:1])
    low = density[0, 0:1] + sum_up + first_down[1:2]
    high = density[0, 1:2] + first_up[1:2] + sum_down
    cells = jnp.concatenate(
        [lame[0] + pair_in[0], shear[0] + pair_in[1], low, high], axis=0
    )
    before, after = halo(cells, "gx")
    along_x = smooth(before, cells, after, spread_x * RADIUS, "smooth_x")
    before, after = halo(along_x, "gy")
    smoothed = smooth(before, along_x, after, spread_y * RADIUS, "smooth_y")
    return smoothed.reshape(3, 2, *smoothed.shape[1:])


def solution(mesh):
    in_specs = (
        P("shot", None, None, None, "gx", "gy"),
        P("shot", None, None, None, "gx", "gy"),
        P("shot", None),
        P("shot", None),
        P("shot", "gx", "gy"),
    )
    out_specs = P(None, "shot", "gx", "gy")
    return jax.shard_map(
        on_device, mesh=mesh, in_specs=in_specs, out_specs=out_specs, check_vma=False
    )
```

```python
import functools

import jax
import jax.numpy as jnp
from jax import lax
from jax.experimental import pallas as pl
from jax.experimental.pallas import tpu as pltpu
from jax.sharding import PartitionSpec as P


RADIUS = 16
MUTE = 32
RZ = 4
ROWS = 16

spread_x = 0.5
spread_y = 0.375


def gradient_kernel(steps, n_out, *refs):
    fwd, adj, small = refs[:3]
    outs = refs[3 : 3 + n_out]
    taper, sems, *bufs = refs[3 + n_out :]
    shot = lax.axis_index("shot")
    half, z = lax.div(shot, RZ), lax.rem(shot, RZ)
    copies = []
    for n, (c0, cn, (x, a, b), _) in enumerate(steps):
        lev = 2 * ((half ^ x) * RZ + (z ^ (a ^ (3 * b))))
        copies.append(
            [
                pltpu.make_async_copy(
                    src.at[0, :, pl.ds(c0, cn), pl.ds(lev, 2)], bufs[n].at[i], sems.at[n, i]
                )
                for i, src in enumerate((fwd, adj))
            ]
        )
    for pair in copies:
        for cp in pair:
            cp.start()
    t0, t1 = small[:, 0:1], small[:, 1:2]
    weights = (-(t0.astype(jnp.float32) / 8.0), -((t1 - t0).astype(jnp.float32) / 8.0))
    inside = small[:, 4:5].astype(jnp.float32)
    shape = taper.shape
    xs = lax.broadcasted_iota(jnp.int32, shape, 0) + lax.axis_index("gx") * shape[0]
    ys = lax.broadcasted_iota(jnp.int32, shape, 1) + lax.axis_index("gy") * shape[1]
    dx = (xs - small[:, 2:3]).astype(jnp.float32)
    dy = (ys - small[:, 3:4]).astype(jnp.float32)
    taper[...] = (1.0 - jnp.exp(-(dx * dx + dy * dy) / (2.0 * MUTE * MUTE))) * inside
    for n, (c0, cn, _, where) in enumerate(steps):
        for cp in copies[n]:
            cp.wait()
        buf = bufs[n]

        def body(lev, carry, buf=buf, c0=c0, cn=cn, where=where):
            for r in range(0, shape[0], ROWS):

                def load(i, k, c):
                    return buf[i, k, c, lev, r : r + ROWS, :].astype(jnp.float32)

                def product(k, c):
                    return load(0, k, c) * load(1, k, c)

                sums = None
                for k, w in enumerate(weights):
                    if c0 == 0:
                        terms = [product(k, 0) + product(k, 1) + product(k, 2)]
                    else:
                        f = [load(0, k, c) for c in range(3)]
                        a = [load(1, k, c) for c in range(3)]
                        terms = []
                        if where[0] is not None:
                            terms.append((f[0] + f[1] + f[2]) * (a[0] + a[1] + a[2]))
                        if where[1] is not None:
                            normal = f[0] * a[0] + f[1] * a[1] + f[2] * a[2]
                            cross = product(k, 3) + product(k, 4) + product(k, 5)
                            terms.append(2.0 * (normal + 2.0 * cross))
                    terms = [t * w for t in terms]
                    sums = terms if sums is None else [s + t for s, t in zip(sums, terms)]
                mask = taper[r : r + ROWS, :]
                for s, (o, i) in zip(sums, [p for p in where if p is not None]):
                    outs[o][i, lev, r : r + ROWS, :] = s * mask
            return carry

        lax.fori_loop(0, 2, body, 0)


def gradient(args, steps, counts):
    wx, wy = args[0].shape[4:]
    hbm, vm = pl.BlockSpec(memory_space=pltpu.HBM), pl.BlockSpec(memory_space=pltpu.VMEM)
    return pl.pallas_call(
        functools.partial(gradient_kernel, steps, len(counts)),
        out_shape=[pltpu.VMEM((c, 2, wx, wy), jnp.float32) for c in counts],
        in_specs=[hbm, hbm, vm],
        out_specs=[vm] * len(counts),
        scratch_shapes=[
            pltpu.VMEM((wx, wy), jnp.float32),
            pltpu.SemaphoreType.DMA((len(steps), 2)),
        ]
        + [pltpu.VMEM((2, 2, s[1], 2, wx, wy), jnp.bfloat16) for s in steps],
        compiler_params=pltpu.CompilerParams(vmem_limit_bytes=24 << 20),
    )(*args)


def band(first, rows, cols, sigma):
    offset = (
        first
        + lax.broadcasted_iota(jnp.int32, (rows, cols), 0)
        - lax.broadcasted_iota(jnp.int32, (rows, cols), 1)
    )
    taps = lax.broadcasted_iota(jnp.int32, (8, 128), 1) - RADIUS

    def bell(at):
        real = at.astype(jnp.float32)
        return jnp.where(
            jnp.abs(at) <= RADIUS, jnp.exp(-real * real / (2.0 * sigma * sigma)), 0.0
        )

    return bell(offset) / jnp.sum(bell(taps)[0:1, :], axis=1, keepdims=True)


def across(cells, weights):
    return lax.dot_general(
        cells,
        weights,
        (((0,), (0,)), ((), ())),
        precision=lax.Precision.HIGHEST,
        preferred_element_type=jnp.float32,
    )


def inner_kernel(sigma, cells, out):
    width = cells.shape[1]
    weights = band(0, width, width, sigma)
    for p in range(cells.shape[0]):
        out[p] = across(cells[p], weights)


def outer_kernel(sigma, axis, inner, even_in, odd_in, out):
    width = inner.shape[2]
    at, count = lax.axis_index(axis), lax.axis_size(axis)
    even = lax.rem(at, 2) == 0
    inside = jnp.logical_and(at > 0, at < count - 1)
    before = band(-RADIUS, RADIUS, width, sigma)
    after = band(width, RADIUS, width, sigma)
    first = jnp.where(even, after, before)
    second = jnp.where(inside, jnp.where(even, before, after), 0.0)
    weights = jnp.concatenate([first, second], axis=0)
    for p in range(inner.shape[0]):
        cells = jnp.concatenate([even_in[p], odd_in[p]], axis=0)
        out[p] = inner[p] + across(cells, weights)


def smooth(cells, axis, sigma, last):
    vm = pl.BlockSpec(memory_space=pltpu.VMEM)
    n, r, c = cells.shape
    count = lax.axis_size(axis)
    even = lax.axis_index(axis) % 2 == 0
    head, tail = cells[:, :RADIUS], cells[:, -RADIUS:]
    swaps = [
        [(i, (i + (1 if i % 2 == k else -1)) % count) for i in range(count)] for k in range(2)
    ]
    first = lax.ppermute(jnp.where(even, tail, head), axis, swaps[0])
    second = lax.ppermute(jnp.where(even, head, tail), axis, swaps[1])
    params = pltpu.CompilerParams(vmem_limit_bytes=16 << 20)
    inner = pl.pallas_call(
        functools.partial(inner_kernel, sigma),
        out_shape=pltpu.VMEM((n, c, r), jnp.float32),
        in_specs=[vm],
        out_specs=vm,
        compiler_params=params,
    )(cells)
    return pl.pallas_call(
        functools.partial(outer_kernel, sigma, axis),
        out_shape=(jax.ShapeDtypeStruct if last else pltpu.VMEM)((n, c, r), jnp.float32),
        in_specs=[vm] * 3,
        out_specs=vm,
        compiler_params=params,
    )(inner, first, second)


def on_device(forward, adjoint, snap_times, sources, aperture):
    forward = pltpu.with_memory_space_constraint(forward, pltpu.HBM)
    adjoint = pltpu.with_memory_space_constraint(adjoint, pltpu.HBM)
    small = jnp.concatenate([snap_times, sources, aperture.reshape(1, 1)], axis=1)
    shots = lax.axis_size("shot")
    flips = {"x": RZ, "a": 1, "b": 3}

    def swap(v, dim):
        return lax.ppermute(v, "shot", [(i, i ^ flips[dim]) for i in range(shots)])

    bits = [(p, q) for p in range(2) for q in range(2)]
    lame_1, shear_1, density_1, lame_high = gradient(
        (forward, adjoint, small),
        [(3, 6, (x, 1, 1), ((0, 2 + x), (1, 2 * x + 1))) for x in range(2)]
        + [(3, 6, (x, 0, 1), ((3, x), (1, 2 * x))) for x in range(2)]
        + [(3, 3, (x, 1, 0), ((0, x), None)) for x in range(2)]
        + [(0, 3, (1, a, b), ((2, 2 * a + b),)) for a, b in bits],
        (4, 4, 4, 2),
    )
    shear_1 = swap(shear_1, "b")
    lame_1 = swap(lame_1, "a")
    density_1 = swap(density_1, "x")
    later = lax.optimization_barrier((small, lame_high))[0]
    lame_low, shear_low, shear_high, density_low, density_high = gradient(
        (forward, adjoint, later),
        [(3, 6, (x, 0, 0), ((0, x), (1 + x, 0))) for x in range(2)]
        + [(3, 6, (x, 1, 0), (None, (1 + x, 1))) for x in range(2)]
        + [(0, 3, (0, a, b), ((3 + a, b),)) for a, b in bits],
        (2, 2, 2, 2, 2),
    )

    def finish(first, low, high, dims):
        second = swap(high + first[2:4], dims[0])
        third = swap(low[1] + first[1] + second[1], dims[1])
        return low[0] + first[0] + second[0] + third

    shear = finish(shear_1, shear_low, shear_high, "xa")
    lame = finish(lame_1, lame_low, lame_high, "bx")
    density = finish(density_1, density_low, density_high, "ab")
    cells = jnp.concatenate([lame, shear, density], axis=0)
    along_x = smooth(cells, "gx", spread_x * RADIUS, False)
    smoothed = smooth(along_x, "gy", spread_y * RADIUS, True)
    return smoothed.reshape(3, 2, *smoothed.shape[1:])


def solution(mesh):
    in_specs = (
        P("shot", None, None, None, "gx", "gy"),
        P("shot", None, None, None, "gx", "gy"),
        P("shot", None),
        P("shot", None),
        P("shot", "gx", "gy"),
    )
    out_specs = P(None, "shot", "gx", "gy")
    return jax.shard_map(on_device, mesh=mesh, in_specs=in_specs, out_specs=out_specs, check_vma=False)
```

```python
import functools

import jax
import jax.numpy as jnp
from jax import lax
from jax.experimental import pallas as pl
from jax.experimental.pallas import tpu as pltpu
from jax.sharding import PartitionSpec as P


RADIUS = 16
MUTE = 32
RZ = 4
ROWS = 16

spread_x = 0.5
spread_y = 0.375


def gradient_kernel(steps, n_out, carried, *refs):
    fwd, adj, small = refs[:3]
    whole = refs[3 : 3 + len(carried)]
    outs = refs[3 + len(carried) :][:n_out]
    taper, sems, *bufs = refs[3 + len(carried) + n_out :]
    shot = lax.axis_index("shot")
    half, z = lax.div(shot, RZ), lax.rem(shot, RZ)
    copies = []
    for n, (c0, cn, (x, a, b), _) in enumerate(steps):
        lev = 2 * ((half ^ x) * RZ + (z ^ (a ^ (3 * b))))
        copies.append(
            [
                pltpu.make_async_copy(
                    src.at[0, :, pl.ds(c0, cn), pl.ds(lev, 2)], bufs[n].at[i], sems.at[n, i]
                )
                for i, src in enumerate((fwd, adj))
            ]
        )
    for pair in copies:
        for cp in pair:
            cp.start()
    for src, (o, i) in zip(whole, carried):
        outs[o][i] = src[0]
    times_etc = small[0]
    t0, t1 = times_etc[:, 0:1], times_etc[:, 1:2]
    weights = (-(t0.astype(jnp.float32) / 8.0), -((t1 - t0).astype(jnp.float32) / 8.0))
    inside = times_etc[:, 4:5].astype(jnp.float32)
    shape = taper.shape
    xs = lax.broadcasted_iota(jnp.int32, shape, 0) + lax.axis_index("gx") * shape[0]
    ys = lax.broadcasted_iota(jnp.int32, shape, 1) + lax.axis_index("gy") * shape[1]
    dx = (xs - times_etc[:, 2:3]).astype(jnp.float32)
    dy = (ys - times_etc[:, 3:4]).astype(jnp.float32)
    taper[...] = (1.0 - jnp.exp(-(dx * dx + dy * dy) / (2.0 * MUTE * MUTE))) * inside
    for n, (c0, cn, _, where) in enumerate(steps):
        for cp in copies[n]:
            cp.wait()
        buf = bufs[n]

        def body(lev, carry, buf=buf, c0=c0, cn=cn, where=where):
            for r in range(0, shape[0], ROWS):

                def load(i, k, c):
                    return buf[i, k, c, lev, r : r + ROWS, :].astype(jnp.float32)

                def product(k, c):
                    return load(0, k, c) * load(1, k, c)

                sums = None
                for k, w in enumerate(weights):
                    if c0 == 0:
                        terms = [product(k, 0) + product(k, 1) + product(k, 2)]
                    else:
                        f = [load(0, k, c) for c in range(3)]
                        a = [load(1, k, c) for c in range(3)]
                        terms = []
                        if where[0] is not None:
                            terms.append((f[0] + f[1] + f[2]) * (a[0] + a[1] + a[2]))
                        if where[1] is not None:
                            normal = f[0] * a[0] + f[1] * a[1] + f[2] * a[2]
                            cross = product(k, 3) + product(k, 4) + product(k, 5)
                            terms.append(2.0 * (normal + 2.0 * cross))
                    terms = [t * w for t in terms]
                    sums = terms if sums is None else [s + t for s, t in zip(sums, terms)]
                mask = taper[r : r + ROWS, :]
                for s, (o, i) in zip(sums, [p for p in where if p is not None]):
                    outs[o][i, lev, r : r + ROWS, :] = s * mask
            return carry

        lax.fori_loop(0, 2, body, 0)


def gradient(args, steps, carried, counts):
    names = list(counts)

    def place(where):
        return None if where is None else (names.index(where[0]), where[1])

    steps = [(*step[:3], tuple(place(w) for w in step[3])) for step in steps]
    kept = [place(where) for _, where in carried]
    wx, wy = args[0].shape[4:]
    hbm, vm = pl.BlockSpec(memory_space=pltpu.HBM), pl.BlockSpec(memory_space=pltpu.VMEM)
    outs = pl.pallas_call(
        functools.partial(gradient_kernel, steps, len(names), kept),
        out_shape=[pltpu.VMEM((c, 2, wx, wy), jnp.float32) for c in counts.values()],
        in_specs=[hbm, hbm] + [vm] * (1 + len(kept)),
        out_specs=[vm] * len(names),
        scratch_shapes=[
            pltpu.VMEM((wx, wy), jnp.float32),
            pltpu.SemaphoreType.DMA((len(steps), 2)),
        ]
        + [pltpu.VMEM((2, 2, s[1], 2, wx, wy), jnp.bfloat16) for s in steps],
        compiler_params=pltpu.CompilerParams(vmem_limit_bytes=12 << 20),
    )(*args, *(src for src, _ in carried))
    return dict(zip(names, outs))


def band(first, rows, cols, sigma):
    offset = (
        first
        + lax.broadcasted_iota(jnp.int32, (rows, cols), 0)
        - lax.broadcasted_iota(jnp.int32, (rows, cols), 1)
    )
    taps = lax.broadcasted_iota(jnp.int32, (8, 128), 1) - RADIUS

    def bell(at):
        real = at.astype(jnp.float32)
        return jnp.where(
            jnp.abs(at) <= RADIUS, jnp.exp(-real * real / (2.0 * sigma * sigma)), 0.0
        )

    return bell(offset) / jnp.sum(bell(taps)[0:1, :], axis=1, keepdims=True)


def three_parts(values, order):
    high = values.astype(jnp.bfloat16)
    low = (values - high.astype(jnp.float32)).astype(jnp.bfloat16)
    return jnp.concatenate([low if part else high for part in order], axis=0)


def across(cells, weights):
    return lax.dot_general(
        three_parts(cells, (0, 0, 1)),
        weights,
        (((0,), (0,)), ((), ())),
        preferred_element_type=jnp.float32,
    )


def inner_kernel(sigma, axis, cells, out, halo_weights):
    width = cells.shape[1]
    weights = three_parts(band(0, width, width, sigma), (0, 1, 0))
    for p in range(cells.shape[0]):
        out[p] = across(cells[p], weights)
    at, count = lax.axis_index(axis), lax.axis_size(axis)
    even = lax.rem(at, 2) == 0
    inside = jnp.logical_and(at > 0, at < count - 1)
    before = band(-RADIUS, RADIUS, width, sigma)
    after = band(width, RADIUS, width, sigma)
    first = jnp.where(even, after, before)
    second = jnp.where(inside, jnp.where(even, before, after), 0.0)
    halo_weights[...] = three_parts(jnp.concatenate([first, second], axis=0), (0, 1, 0))


def outer_kernel(inner, weights, even_in, odd_in, out):
    for p in range(inner.shape[0]):
        cells = jnp.concatenate([even_in[p], odd_in[p]], axis=0)
        out[p] = inner[p] + across(cells, weights[...])


def smooth(cells, axis, sigma, last):
    vm = pl.BlockSpec(memory_space=pltpu.VMEM)
    n, r, c = cells.shape
    count = lax.axis_size(axis)
    even = lax.axis_index(axis) % 2 == 0
    head, tail = cells[:, :RADIUS], cells[:, -RADIUS:]
    swaps = [
        [(i, (i + (1 if i % 2 == k else -1)) % count) for i in range(count)] for k in range(2)
    ]
    first = lax.ppermute(jnp.where(even, tail, head), axis, swaps[0])
    second = lax.ppermute(jnp.where(even, head, tail), axis, swaps[1])
    params = pltpu.CompilerParams(vmem_limit_bytes=16 << 20)
    inner, weights = pl.pallas_call(
        functools.partial(inner_kernel, sigma, axis),
        out_shape=[
            pltpu.VMEM((n, c, r), jnp.float32),
            pltpu.VMEM((6 * RADIUS, r), jnp.bfloat16),
        ],
        in_specs=[vm],
        out_specs=[vm] * 2,
        compiler_params=params,
    )(cells)
    return pl.pallas_call(
        outer_kernel,
        out_shape=(jax.ShapeDtypeStruct if last else pltpu.VMEM)((n, c, r), jnp.float32),
        in_specs=[vm] * 4,
        out_specs=vm,
        compiler_params=params,
    )(inner, weights, first, second)


def add_up_kernel(mine_1, mine_0, in10, in01_1, sent, rest):
    sent[...] = mine_1[0] + in10[1] + in01_1[...]
    rest[...] = mine_0[0] + in10[0]


def add_up(mine_1, mine_0, in10, in01_1):
    vm = pl.BlockSpec(memory_space=pltpu.VMEM)
    return pl.pallas_call(
        add_up_kernel,
        out_shape=[pltpu.VMEM(in01_1.shape, jnp.float32)] * 2,
        in_specs=[vm] * 4,
        out_specs=[vm] * 2,
        compiler_params=pltpu.CompilerParams(vmem_limit_bytes=4 << 20),
        name="add_up",
    )(mine_1, mine_0, pltpu.with_memory_space_constraint(in10, pltpu.VMEM), in01_1)


def on_device(forward, adjoint, snap_times, sources, aperture):
    forward = pltpu.with_memory_space_constraint(forward, pltpu.HBM)
    adjoint = pltpu.with_memory_space_constraint(adjoint, pltpu.HBM)
    small = jnp.concatenate([snap_times[None], sources[None], aperture], axis=2)
    shots = lax.axis_size("shot")
    flips = {"x": RZ, "a": 1, "b": 3}

    def swap(v, dim):
        return lax.ppermute(v, "shot", [(i, i ^ flips[dim]) for i in range(shots)])

    args = (forward, adjoint, small)
    v = gradient(
        args,
        [
            (3, 6, (1, 1, 1), (("lame11", 1), ("shear11", 1))),
            (3, 6, (0, 1, 1), (("lame11", 0), ("shear10_1", 0))),
            (3, 6, (1, 0, 1), (("lame01_1", 0), ("shear11", 0))),
            (0, 3, (1, 1, 0), (("density11", 0),)),
            (0, 3, (1, 1, 1), (("density11", 1),)),
        ],
        [],
        {"lame11": 2, "shear11": 2, "density11": 2, "shear10_1": 1, "lame01_1": 1},
    )
    shear11 = swap(v["shear11"], "b")
    lame11 = swap(v["lame11"], "a")
    density11 = swap(v["density11"], "x")
    v |= gradient(
        args,
        [
            (3, 6, (0, 0, 1), (("lame01_0", 0), ("shear10", 0))),
            (3, 6, (0, 1, 0), (("lame10", 0), ("shear00_1", 0))),
            (3, 6, (1, 1, 0), (("lame10", 1), ("shear01_1", 0))),
            (0, 3, (1, 0, 0), (("density10", 0),)),
            (0, 3, (1, 0, 1), (("density10", 1),)),
        ],
        [(v["shear10_1"], ("shear10", 1))],
        {
            "lame10": 2, "shear10": 2, "density10": 2,
            "lame01_0": 1, "shear00_1": 1, "shear01_1": 1,
        },
    )
    shear10 = swap(v["shear10"], "b")
    lame10 = swap(v["lame10"], "a")
    density10 = swap(v["density10"], "x")
    later = lax.optimization_barrier((small, v["lame10"]))[0]
    v |= gradient(
        (forward, adjoint, later),
        [
            (3, 6, (1, 0, 0), (("lame00_1", 0), ("shear01_0", 0))),
            (0, 3, (0, 1, 0), (("density01_0", 0),)),
            (0, 3, (0, 1, 1), (("density01_1", 0),)),
            (3, 6, (0, 0, 0), (("lame00_0", 0), ("shear00_0", 0))),
            (0, 3, (0, 0, 0), (("density00_0", 0),)),
            (0, 3, (0, 0, 1), (("density00_1", 0),)),
        ],
        [],
        {
            "lame00_0": 1, "lame00_1": 1, "shear00_0": 1, "shear01_0": 1,
            "density00_0": 1, "density00_1": 1, "density01_0": 1, "density01_1": 1,
        },
    )

    def finish(name, in11, in10, dims):
        def mine(bits):
            return v[name + bits][0]

        in01_1 = swap(mine("01_1") + in11[1], dims[0])
        in01_0 = swap(mine("01_0") + in11[0], dims[0])
        sent, rest = add_up(v[name + "00_1"], v[name + "00_0"], in10, in01_1)
        return rest + in01_0 + swap(sent, dims[1])

    shear = finish("shear", shear11, shear10, "xa")
    lame = finish("lame", lame11, lame10, "bx")
    density = finish("density", density11, density10, "ab")
    cells = jnp.concatenate([lame, shear, density], axis=0)
    along_x = smooth(cells, "gx", spread_x * RADIUS, False)
    smoothed = smooth(along_x, "gy", spread_y * RADIUS, True)
    return smoothed.reshape(3, 2, *smoothed.shape[1:])


def solution(mesh):
    in_specs = (
        P("shot", None, None, None, "gx", "gy"),
        P("shot", None, None, None, "gx", "gy"),
        P("shot", None),
        P("shot", None),
        P("shot", "gx", "gy"),
    )
    out_specs = P(None, "shot", "gx", "gy")
    return jax.shard_map(on_device, mesh=mesh, in_specs=in_specs, out_specs=out_specs, check_vma=False)
```

```python
import functools

import jax
import jax.numpy as jnp
from jax import lax
from jax.experimental import pallas as pl
from jax.experimental.pallas import tpu as pltpu
from jax.sharding import PartitionSpec as P


RADIUS = 16
MUTE = 32
RZ = 4
ROWS = 16

spread_x = 0.5
spread_y = 0.375


def gradient_kernel(steps, n_out, resident, first, *refs):
    fwd, adj = refs[:2]
    if first:
        times, sources, aperture, *refs = refs[2:]
        outs, refs = refs[:n_out], refs[n_out:]
        taper, factors, sems, time_cells, source_cells, small_sems, *bufs = refs
    else:
        taper, factors, *refs = refs[2:]
        outs, refs = refs[:n_out], refs[n_out:]
        sems, *bufs = refs
    streamed = [i for i in range(2) if not resident[i]]
    shot = lax.axis_index("shot")
    half, z = lax.div(shot, RZ), lax.rem(shot, RZ)
    if first:
        smalls = [
            pltpu.make_async_copy(times, time_cells, small_sems.at[0]),
            pltpu.make_async_copy(sources, source_cells, small_sems.at[1]),
        ]
        for cp in smalls:
            cp.start()
    copies, levels = [], []
    for n, (c0, cn, (x, a, b), _) in enumerate(steps):
        lev = 2 * ((half ^ x) * RZ + (z ^ (a ^ (3 * b))))
        levels.append(lev)
        copies.append(
            [
                pltpu.make_async_copy(
                    (fwd, adj)[i].at[0, :, pl.ds(c0, cn), pl.ds(lev, 2)],
                    bufs[n].at[slot],
                    sems.at[n, slot],
                )
                for slot, i in enumerate(streamed)
            ]
        )
    for pair in copies:
        for cp in pair:
            cp.start()
    shape = taper.shape
    if first:
        for cp in smalls:
            cp.wait()
        t0, t1 = time_cells[:, 0:1], time_cells[:, 1:2]
        for k, step in enumerate((t0, t1 - t0)):
            factors[k] = jnp.broadcast_to(-(step.astype(jnp.float32) / 8.0), factors.shape[1:])
        inside = aperture[0, 0, 0].astype(jnp.float32)
        xs = lax.broadcasted_iota(jnp.int32, shape, 0) + lax.axis_index("gx") * shape[0]
        ys = lax.broadcasted_iota(jnp.int32, shape, 1) + lax.axis_index("gy") * shape[1]
        dx = (xs - source_cells[:, 0:1]).astype(jnp.float32)
        dy = (ys - source_cells[:, 1:2]).astype(jnp.float32)
        taper[...] = (1.0 - jnp.exp(-(dx * dx + dy * dy) / (2.0 * MUTE * MUTE))) * inside
    weights = [factors[k] for k in range(2)]
    for n, (c0, cn, _, where) in enumerate(steps):
        for cp in copies[n]:
            cp.wait()
        buf = bufs[n] if streamed else None

        def body(lev, carry, buf=buf, first=levels[n], c0=c0, cn=cn, where=where):
            for r in range(0, shape[0], ROWS):

                def load(i, k, c):
                    if resident[i]:
                        cells = (fwd, adj)[i][0, k, c0 + c, first + lev, r : r + ROWS, :]
                    else:
                        cells = buf[streamed.index(i), k, c, lev, r : r + ROWS, :]
                    return cells.astype(jnp.float32)

                def product(k, c):
                    return load(0, k, c) * load(1, k, c)

                sums = None
                for k, w in enumerate(weights):
                    if c0 == 0:
                        terms = [product(k, 0) + product(k, 1) + product(k, 2)]
                    else:
                        f = [load(0, k, c) for c in range(3)]
                        a = [load(1, k, c) for c in range(3)]
                        terms = []
                        if where[0] is not None:
                            terms.append((f[0] + f[1] + f[2]) * (a[0] + a[1] + a[2]))
                        if where[1] is not None:
                            normal = f[0] * a[0] + f[1] * a[1] + f[2] * a[2]
                            cross = product(k, 3) + product(k, 4) + product(k, 5)
                            terms.append(2.0 * (normal + 2.0 * cross))
                    terms = [t * w for t in terms]
                    sums = terms if sums is None else [s + t for s, t in zip(sums, terms)]
                mask = taper[r : r + ROWS, :]
                for s, (o, i) in zip(sums, [p for p in where if p is not None]):
                    outs[o][i, lev, r : r + ROWS, :] = s * mask
            return carry

        lax.fori_loop(0, 2, body, 0)


def gradient(args, resident, steps, counts):
    names = list(counts)

    def place(where):
        return None if where is None else (names.index(where[0]), where[1])

    steps = [(*step[:3], tuple(place(w) for w in step[3])) for step in steps]
    wx, wy = args[0].shape[4:]
    vm = pl.BlockSpec(memory_space=pltpu.VMEM)
    first = len(args) == 5
    spaces = [pltpu.VMEM if r else pltpu.HBM for r in resident]
    waves = [pltpu.with_memory_space_constraint(a, m) for a, m in zip(args[:2], spaces)]
    rest = list(args[2:])
    specs = [vm, vm]
    outs = [pltpu.VMEM((c, 2, wx, wy), jnp.float32) for c in counts.values()]
    small_scratch = []
    if first:
        rest[:2] = [pltpu.with_memory_space_constraint(a, pltpu.HBM) for a in rest[:2]]
        specs = [pl.BlockSpec(memory_space=m) for m in (pltpu.HBM, pltpu.HBM, pltpu.SMEM)]
        outs += [pltpu.VMEM((wx, wy), jnp.float32), pltpu.VMEM((2, ROWS, wy), jnp.float32)]
        small_scratch = [pltpu.VMEM(a.shape, jnp.int32) for a in rest[:2]]
        small_scratch.append(pltpu.SemaphoreType.DMA((2,)))
    streams = 2 - sum(resident)
    results = pl.pallas_call(
        functools.partial(gradient_kernel, steps, len(names), resident, first),
        out_shape=outs,
        in_specs=[pl.BlockSpec(memory_space=m) for m in spaces] + specs,
        out_specs=[vm] * len(outs),
        scratch_shapes=[pltpu.SemaphoreType.DMA((len(steps), max(streams, 1)))]
        + small_scratch
        + [pltpu.VMEM((streams, 2, s[1], 2, wx, wy), jnp.bfloat16) for s in steps if streams],
        compiler_params=pltpu.CompilerParams(vmem_limit_bytes=12 << 20),
    )(*waves, *rest)
    return dict(zip(names + ["taper", "factors"], results))


def band(first, rows, cols, sigma):
    offset = (
        first
        + lax.broadcasted_iota(jnp.int32, (rows, cols), 0)
        - lax.broadcasted_iota(jnp.int32, (rows, cols), 1)
    )
    taps = lax.broadcasted_iota(jnp.int32, (8, 128), 1) - RADIUS

    def bell(at):
        real = at.astype(jnp.float32)
        return jnp.where(
            jnp.abs(at) <= RADIUS, jnp.exp(-real * real / (2.0 * sigma * sigma)), 0.0
        )

    return bell(offset) / jnp.sum(bell(taps)[0:1, :], axis=1, keepdims=True)


def three_parts(values, order):
    high = values.astype(jnp.bfloat16)
    low = (values - high.astype(jnp.float32)).astype(jnp.bfloat16)
    return jnp.concatenate([low if part else high for part in order], axis=0)


def across(cells, weights):
    return lax.dot_general(
        three_parts(cells, (0, 0, 1)),
        weights,
        (((0,), (0,)), ((), ())),
        preferred_element_type=jnp.float32,
    )


def inner_kernel(sigma, axis, cells, out, halo_weights):
    width = cells.shape[1]
    weights = three_parts(band(0, width, width, sigma), (0, 1, 0))
    for p in range(cells.shape[0]):
        out[p] = across(cells[p], weights)
    at, count = lax.axis_index(axis), lax.axis_size(axis)
    even = lax.rem(at, 2) == 0
    inside = jnp.logical_and(at > 0, at < count - 1)
    before = band(-RADIUS, RADIUS, width, sigma)
    after = band(width, RADIUS, width, sigma)
    first = jnp.where(even, after, before)
    second = jnp.where(inside, jnp.where(even, before, after), 0.0)
    halo_weights[...] = three_parts(jnp.concatenate([first, second], axis=0), (0, 1, 0))


def outer_kernel(inner, weights, even_in, odd_in, out):
    for p in range(inner.shape[0]):
        cells = jnp.concatenate([even_in[p], odd_in[p]], axis=0)
        out[p] = inner[p] + across(cells, weights[...])


def smooth(cells, axis, sigma, last):
    vm = pl.BlockSpec(memory_space=pltpu.VMEM)
    n, r, c = cells.shape
    count = lax.axis_size(axis)
    even = lax.axis_index(axis) % 2 == 0
    head, tail = cells[:, :RADIUS], cells[:, -RADIUS:]
    swaps = [
        [(i, (i + (1 if i % 2 == k else -1)) % count) for i in range(count)] for k in range(2)
    ]
    first = lax.ppermute(jnp.where(even, tail, head), axis, swaps[0])
    second = lax.ppermute(jnp.where(even, head, tail), axis, swaps[1])
    params = pltpu.CompilerParams(vmem_limit_bytes=16 << 20)
    inner, weights = pl.pallas_call(
        functools.partial(inner_kernel, sigma, axis),
        out_shape=[
            pltpu.VMEM((n, c, r), jnp.float32),
            pltpu.VMEM((6 * RADIUS, r), jnp.bfloat16),
        ],
        in_specs=[vm],
        out_specs=[vm] * 2,
        compiler_params=params,
    )(cells)
    return pl.pallas_call(
        outer_kernel,
        out_shape=(jax.ShapeDtypeStruct if last else pltpu.VMEM)((n, c, r), jnp.float32),
        in_specs=[vm] * 4,
        out_specs=vm,
        compiler_params=params,
    )(inner, weights, first, second)


def add_up_kernel(mine_1, mine_0, in10, in01_1, sent, rest):
    sent[...] = mine_1[0] + in10[1] + in01_1[...]
    rest[...] = mine_0[0] + in10[0]


def add_up(mine_1, mine_0, in10, in01_1):
    vm = pl.BlockSpec(memory_space=pltpu.VMEM)
    return pl.pallas_call(
        add_up_kernel,
        out_shape=[pltpu.VMEM(in01_1.shape, jnp.float32)] * 2,
        in_specs=[vm] * 4,
        out_specs=[vm] * 2,
        compiler_params=pltpu.CompilerParams(vmem_limit_bytes=4 << 20),
        name="add_up",
    )(mine_1, mine_0, pltpu.with_memory_space_constraint(in10, pltpu.VMEM), in01_1)


def on_device(forward, adjoint, snap_times, sources, aperture):
    shots = lax.axis_size("shot")
    flips = {"x": RZ, "a": 1, "b": 3}

    def swap(v, dim):
        return lax.ppermute(v, "shot", [(i, i ^ flips[dim]) for i in range(shots)])

    args = (forward, adjoint, snap_times, sources, aperture)
    v = gradient(
        args,
        (False, False),
        [
            (3, 6, (1, 1, 1), (("lame11", 1), ("shear11", 1))),
            (3, 3, (0, 1, 1), (("lame11", 0), None)),
            (3, 6, (1, 0, 1), (("lame01_1", 0), ("shear11", 0))),
            (0, 3, (1, 1, 0), (("density11", 0),)),
            (0, 3, (1, 1, 1), (("density11", 1),)),
        ],
        {"lame11": 2, "shear11": 2, "density11": 2, "lame01_1": 1},
    )
    shear11 = swap(v["shear11"], "b")
    lame11 = swap(v["lame11"], "a")
    density11 = swap(v["density11"], "x")
    v |= gradient(
        (forward, adjoint, v["taper"], v["factors"]),
        (True, True),
        [
            (3, 6, (0, 0, 1), (("lame01_0", 0), ("shear10", 0))),
            (3, 6, (0, 1, 1), (None, ("shear10", 1))),
            (3, 6, (0, 1, 0), (("lame10", 0), ("shear00_1", 0))),
            (3, 6, (1, 1, 0), (("lame10", 1), ("shear01_1", 0))),
            (0, 3, (1, 0, 0), (("density10", 0),)),
            (0, 3, (1, 0, 1), (("density10", 1),)),
        ],
        {
            "lame10": 2, "shear10": 2, "density10": 2,
            "lame01_0": 1, "shear00_1": 1, "shear01_1": 1,
        },
    )
    shear10 = swap(v["shear10"], "b")
    lame10 = swap(v["lame10"], "a")
    density10 = swap(v["density10"], "x")
    taper = lax.optimization_barrier((v["taper"], v["lame10"]))[0]
    v |= gradient(
        (forward, adjoint, taper, v["factors"]),
        (True, True),
        [
            (3, 6, (1, 0, 0), (("lame00_1", 0), ("shear01_0", 0))),
            (0, 3, (0, 1, 0), (("density01_0", 0),)),
            (0, 3, (0, 1, 1), (("density01_1", 0),)),
            (3, 6, (0, 0, 0), (("lame00_0", 0), ("shear00_0", 0))),
            (0, 3, (0, 0, 0), (("density00_0", 0),)),
            (0, 3, (0, 0, 1), (("density00_1", 0),)),
        ],
        {
            "lame00_0": 1, "lame00_1": 1, "shear00_0": 1, "shear01_0": 1,
            "density00_0": 1, "density00_1": 1, "density01_0": 1, "density01_1": 1,
        },
    )

    def finish(name, in11, in10, dims):
        def mine(bits):
            return v[name + bits][0]

        in01_1 = swap(mine("01_1") + in11[1], dims[0])
        in01_0 = swap(mine("01_0") + in11[0], dims[0])
        sent, rest = add_up(v[name + "00_1"], v[name + "00_0"], in10, in01_1)
        return rest + in01_0 + swap(sent, dims[1])

    shear = finish("shear", shear11, shear10, "xa")
    lame = finish("lame", lame11, lame10, "bx")
    density = finish("density", density11, density10, "ab")
    cells = jnp.concatenate([lame, shear, density], axis=0)
    along_x = smooth(cells, "gx", spread_x * RADIUS, False)
    smoothed = smooth(along_x, "gy", spread_y * RADIUS, True)
    return smoothed.reshape(3, 2, *smoothed.shape[1:])


def solution(mesh):
    in_specs = (
        P("shot", None, None, None, "gx", "gy"),
        P("shot", None, None, None, "gx", "gy"),
        P("shot", None),
        P("shot", None),
        P("shot", "gx", "gy"),
    )
    out_specs = P(None, "shot", "gx", "gy")
    return jax.shard_map(on_device, mesh=mesh, in_specs=in_specs, out_specs=out_specs, check_vma=False)
```

```python
import functools

import jax
import jax.numpy as jnp
from jax import lax
from jax.experimental import pallas as pl
from jax.experimental.pallas import tpu as pltpu
from jax.sharding import PartitionSpec as P


RADIUS = 16
MUTE = 32
RZ = 4
ROWS = 16

spread_x = 0.5
spread_y = 0.375


def gradient_kernel(steps, n_out, resident, first, *refs):
    fwd, adj = refs[:2]
    if first:
        times, sources, aperture, *refs = refs[2:]
        outs, refs = refs[:n_out], refs[n_out:]
        taper, factors, sems, time_cells, source_cells, small_sems, *bufs = refs
    else:
        taper, factors, *refs = refs[2:]
        outs, refs = refs[:n_out], refs[n_out:]
        sems, *bufs = refs
    streamed = [i for i in range(2) if not resident[i]]
    shot = lax.axis_index("shot")
    half, z = lax.div(shot, RZ), lax.rem(shot, RZ)
    if first:
        smalls = [
            pltpu.make_async_copy(times, time_cells, small_sems.at[0]),
            pltpu.make_async_copy(sources, source_cells, small_sems.at[1]),
        ]
        for cp in smalls:
            cp.start()
    copies, levels = [], []
    for n, (c0, cn, (x, a, b), _) in enumerate(steps):
        lev = 2 * ((half ^ x) * RZ + (z ^ (a ^ (3 * b))))
        levels.append(lev)
        copies.append(
            [
                pltpu.make_async_copy(
                    (fwd, adj)[i].at[0, :, pl.ds(c0, cn), pl.ds(lev, 2)],
                    bufs[n].at[slot],
                    sems.at[n, slot],
                )
                for slot, i in enumerate(streamed)
            ]
        )
    for pair in copies:
        for cp in pair:
            cp.start()
    shape = taper.shape
    if first:
        for cp in smalls:
            cp.wait()
        t0, t1 = time_cells[:, 0:1], time_cells[:, 1:2]
        for k, step in enumerate((t0, t1 - t0)):
            factors[k] = jnp.broadcast_to(-(step.astype(jnp.float32) / 8.0), factors.shape[1:])
        inside = aperture[0, 0, 0].astype(jnp.float32)
        xs = lax.broadcasted_iota(jnp.int32, shape, 0) + lax.axis_index("gx") * shape[0]
        ys = lax.broadcasted_iota(jnp.int32, shape, 1) + lax.axis_index("gy") * shape[1]
        dx = (xs - source_cells[:, 0:1]).astype(jnp.float32)
        dy = (ys - source_cells[:, 1:2]).astype(jnp.float32)
        taper[...] = (1.0 - jnp.exp(-(dx * dx + dy * dy) / (2.0 * MUTE * MUTE))) * inside
    weights = [factors[k] for k in range(2)]
    for n, (c0, cn, _, where) in enumerate(steps):
        for cp in copies[n]:
            cp.wait()
        buf = bufs[n] if streamed else None

        def body(lev, carry, buf=buf, first=levels[n], c0=c0, cn=cn, where=where):
            for r in range(0, shape[0], ROWS):

                def load(i, k, c):
                    if resident[i]:
                        cells = (fwd, adj)[i][0, k, c0 + c, first + lev, r : r + ROWS, :]
                    else:
                        cells = buf[streamed.index(i), k, c, lev, r : r + ROWS, :]
                    return cells.astype(jnp.float32)

                def product(k, c):
                    return load(0, k, c) * load(1, k, c)

                sums = None
                for k, w in enumerate(weights):
                    if c0 == 0:
                        terms = [product(k, 0) + product(k, 1) + product(k, 2)]
                    else:
                        f = [load(0, k, c) for c in range(3)]
                        a = [load(1, k, c) for c in range(3)]
                        terms = []
                        if where[0] is not None:
                            terms.append((f[0] + f[1] + f[2]) * (a[0] + a[1] + a[2]))
                        if where[1] is not None:
                            normal = f[0] * a[0] + f[1] * a[1] + f[2] * a[2]
                            cross = product(k, 3) + product(k, 4) + product(k, 5)
                            terms.append(2.0 * (normal + 2.0 * cross))
                    terms = [t * w for t in terms]
                    sums = terms if sums is None else [s + t for s, t in zip(sums, terms)]
                mask = taper[r : r + ROWS, :]
                for s, (o, i) in zip(sums, [p for p in where if p is not None]):
                    outs[o][i, lev, r : r + ROWS, :] = s * mask
            return carry

        lax.fori_loop(0, 2, body, 0)


def gradient(args, resident, steps, counts):
    names = list(counts)

    def place(where):
        return None if where is None else (names.index(where[0]), where[1])

    steps = [(*step[:3], tuple(place(w) for w in step[3])) for step in steps]
    wx, wy = args[0].shape[4:]
    vm = pl.BlockSpec(memory_space=pltpu.VMEM)
    first = len(args) == 5
    spaces = [pltpu.VMEM if r else pltpu.HBM for r in resident]
    waves = [pltpu.with_memory_space_constraint(a, m) for a, m in zip(args[:2], spaces)]
    rest = list(args[2:])
    specs = [vm, vm]
    outs = [pltpu.VMEM((c, 2, wx, wy), jnp.float32) for c in counts.values()]
    small_scratch = []
    if first:
        rest[:2] = [pltpu.with_memory_space_constraint(a, pltpu.HBM) for a in rest[:2]]
        specs = [pl.BlockSpec(memory_space=m) for m in (pltpu.HBM, pltpu.HBM, pltpu.SMEM)]
        outs += [pltpu.VMEM((wx, wy), jnp.float32), pltpu.VMEM((2, ROWS, wy), jnp.float32)]
        small_scratch = [pltpu.VMEM(a.shape, jnp.int32) for a in rest[:2]]
        small_scratch.append(pltpu.SemaphoreType.DMA((2,)))
    streams = 2 - sum(resident)
    results = pl.pallas_call(
        functools.partial(gradient_kernel, steps, len(names), resident, first),
        out_shape=outs,
        in_specs=[pl.BlockSpec(memory_space=m) for m in spaces] + specs,
        out_specs=[vm] * len(outs),
        scratch_shapes=[pltpu.SemaphoreType.DMA((len(steps), max(streams, 1)))]
        + small_scratch
        + [pltpu.VMEM((streams, 2, s[1], 2, wx, wy), jnp.bfloat16) for s in steps if streams],
        compiler_params=pltpu.CompilerParams(vmem_limit_bytes=12 << 20),
    )(*waves, *rest)
    return dict(zip(names + ["taper", "factors"], results))


def band(first, rows, cols, sigma):
    offset = (
        first
        + lax.broadcasted_iota(jnp.int32, (rows, cols), 0)
        - lax.broadcasted_iota(jnp.int32, (rows, cols), 1)
    )
    taps = lax.broadcasted_iota(jnp.int32, (8, 128), 1) - RADIUS

    def bell(at):
        real = at.astype(jnp.float32)
        return jnp.where(
            jnp.abs(at) <= RADIUS, jnp.exp(-real * real / (2.0 * sigma * sigma)), 0.0
        )

    return bell(offset) / jnp.sum(bell(taps)[0:1, :], axis=1, keepdims=True)


def three_parts(values, order):
    high = values.astype(jnp.bfloat16)
    low = (values - high.astype(jnp.float32)).astype(jnp.bfloat16)
    return jnp.concatenate([low if part else high for part in order], axis=0)


def across(cells, weights):
    return lax.dot_general(
        three_parts(cells, (0, 0, 1)),
        weights,
        (((0,), (0,)), ((), ())),
        preferred_element_type=jnp.float32,
    )


def inner_kernel(sigma, axis, cells, out, halo_weights):
    width = cells.shape[1]
    weights = three_parts(band(0, width, width, sigma), (0, 1, 0))
    for p in range(cells.shape[0]):
        out[p] = across(cells[p], weights)
    at, count = lax.axis_index(axis), lax.axis_size(axis)
    even = lax.rem(at, 2) == 0
    inside = jnp.logical_and(at > 0, at < count - 1)
    before = band(-RADIUS, RADIUS, width, sigma)
    after = band(width, RADIUS, width, sigma)
    first = jnp.where(even, after, before)
    second = jnp.where(inside, jnp.where(even, before, after), 0.0)
    halo_weights[...] = three_parts(jnp.concatenate([first, second], axis=0), (0, 1, 0))


def outer_kernel(inner, weights, even_in, odd_in, out):
    for p in range(inner.shape[0]):
        cells = jnp.concatenate([even_in[p], odd_in[p]], axis=0)
        out[p] = inner[p] + across(cells, weights[...])


def smooth(cells, axis, sigma, last):
    vm = pl.BlockSpec(memory_space=pltpu.VMEM)
    n, r, c = cells.shape
    count = lax.axis_size(axis)
    even = lax.axis_index(axis) % 2 == 0
    head, tail = cells[:, :RADIUS], cells[:, -RADIUS:]
    swaps = [
        [(i, (i + (1 if i % 2 == k else -1)) % count) for i in range(count)] for k in range(2)
    ]
    first = lax.ppermute(jnp.where(even, tail, head), axis, swaps[0])
    second = lax.ppermute(jnp.where(even, head, tail), axis, swaps[1])
    params = pltpu.CompilerParams(vmem_limit_bytes=16 << 20)
    inner, weights = pl.pallas_call(
        functools.partial(inner_kernel, sigma, axis),
        out_shape=[
            pltpu.VMEM((n, c, r), jnp.float32),
            pltpu.VMEM((6 * RADIUS, r), jnp.bfloat16),
        ],
        in_specs=[vm],
        out_specs=[vm] * 2,
        compiler_params=params,
    )(cells)
    return pl.pallas_call(
        outer_kernel,
        out_shape=(jax.ShapeDtypeStruct if last else pltpu.VMEM)((n, c, r), jnp.float32),
        in_specs=[vm] * 4,
        out_specs=vm,
        compiler_params=params,
    )(inner, weights, first, second)


def add_up_kernel(mine_1, mine_0, in10, in01_1, sent, rest):
    sent[...] = mine_1[0] + in10[1] + in01_1[...]
    rest[...] = mine_0[0] + in10[0]


def add_up(mine_1, mine_0, in10, in01_1):
    vm = pl.BlockSpec(memory_space=pltpu.VMEM)
    return pl.pallas_call(
        add_up_kernel,
        out_shape=[pltpu.VMEM(in01_1.shape, jnp.float32)] * 2,
        in_specs=[vm] * 4,
        out_specs=[vm] * 2,
        compiler_params=pltpu.CompilerParams(vmem_limit_bytes=4 << 20),
        name="add_up",
    )(mine_1, mine_0, pltpu.with_memory_space_constraint(in10, pltpu.VMEM), in01_1)


def on_device(forward, adjoint, snap_times, sources, aperture):
    shots = lax.axis_size("shot")
    flips = {"x": RZ, "a": 1, "b": 3}

    def swap(v, dim):
        return lax.ppermute(v, "shot", [(i, i ^ flips[dim]) for i in range(shots)])

    args = (forward, adjoint, snap_times, sources, aperture)
    v = gradient(
        args,
        (False, False),
        [
            (3, 6, (1, 1, 1), (("lame11", 1), ("shear11", 1))),
            (3, 3, (0, 1, 1), (("lame11", 0), None)),
            (3, 6, (1, 0, 1), (("lame01_1", 0), ("shear11", 0))),
            (0, 3, (1, 1, 0), (("density11", 0),)),
            (0, 3, (1, 1, 1), (("density11", 1),)),
        ],
        {"lame11": 2, "shear11": 2, "density11": 2, "lame01_1": 1},
    )
    shear11 = swap(v["shear11"], "b")
    lame11 = swap(v["lame11"], "a")
    density11 = swap(v["density11"], "x")
    v |= gradient(
        (forward, adjoint, v["taper"], v["factors"]),
        (True, False),
        [
            (3, 6, (0, 0, 1), (None, ("shear10", 0))),
            (3, 6, (0, 1, 1), (None, ("shear10", 1))),
            (3, 3, (0, 1, 0), (("lame10", 0), None)),
            (3, 3, (1, 1, 0), (("lame10", 1), None)),
            (0, 3, (1, 0, 0), (("density10", 0),)),
            (0, 3, (1, 0, 1), (("density10", 1),)),
        ],
        {
            "lame10": 2, "shear10": 2, "density10": 2,
        },
    )
    shear10 = swap(v["shear10"], "b")
    lame10 = swap(v["lame10"], "a")
    density10 = swap(v["density10"], "x")
    taper = lax.optimization_barrier((v["taper"], v["lame10"]))[0]
    v |= gradient(
        (forward, adjoint, taper, v["factors"]),
        (True, True),
        [
            (3, 3, (0, 0, 1), (("lame01_0", 0), None)),
            (3, 6, (0, 1, 0), (None, ("shear00_1", 0))),
            (3, 6, (1, 1, 0), (None, ("shear01_1", 0))),
            (3, 6, (1, 0, 0), (("lame00_1", 0), ("shear01_0", 0))),
            (0, 3, (0, 1, 0), (("density01_0", 0),)),
            (0, 3, (0, 1, 1), (("density01_1", 0),)),
            (3, 6, (0, 0, 0), (("lame00_0", 0), ("shear00_0", 0))),
            (0, 3, (0, 0, 0), (("density00_0", 0),)),
            (0, 3, (0, 0, 1), (("density00_1", 0),)),
        ],
        {
            "lame00_0": 1, "lame00_1": 1, "lame01_0": 1,
            "shear00_0": 1, "shear00_1": 1, "shear01_0": 1, "shear01_1": 1,
            "density00_0": 1, "density00_1": 1, "density01_0": 1, "density01_1": 1,
        },
    )

    def finish(name, in11, in10, dims):
        def mine(bits):
            return v[name + bits][0]

        in01_1 = swap(mine("01_1") + in11[1], dims[0])
        in01_0 = swap(mine("01_0") + in11[0], dims[0])
        sent, rest = add_up(v[name + "00_1"], v[name + "00_0"], in10, in01_1)
        return rest + in01_0 + swap(sent, dims[1])

    shear = finish("shear", shear11, shear10, "xa")
    lame = finish("lame", lame11, lame10, "bx")
    density = finish("density", density11, density10, "ab")
    cells = jnp.concatenate([lame, shear, density], axis=0)
    along_x = smooth(cells, "gx", spread_x * RADIUS, False)
    smoothed = smooth(along_x, "gy", spread_y * RADIUS, True)
    return smoothed.reshape(3, 2, *smoothed.shape[1:])


def solution(mesh):
    in_specs = (
        P("shot", None, None, None, "gx", "gy"),
        P("shot", None, None, None, "gx", "gy"),
        P("shot", None),
        P("shot", None),
        P("shot", "gx", "gy"),
    )
    out_specs = P(None, "shot", "gx", "gy")
    return jax.shard_map(on_device, mesh=mesh, in_specs=in_specs, out_specs=out_specs, check_vma=False)
```
